256 devices in a mesh: rep: 2 (over core), dp: 128 (over x, y, z).
Axes of the slice: x: 4, y: 4, z: 8, core: 2. Of those that a mesh axis runs over, the one named last changes fastest.
Arguments:
- x: bfloat16 [256, 2048, 1024], P(('rep', 'dp')), parts along dimension 0
- dy: bfloat16 [256, 2048, 1024], P(('rep', 'dp')), parts along dimension 0
- wq: bfloat16 [1, 1024, 1024], P(None, 'dp')
- wk: bfloat16 [1, 1024, 1024], P(None, 'dp')
- wv: bfloat16 [1, 1024, 1024], P(None, 'dp')
- wo: bfloat16 [1, 1024, 1024], P(None, 'dp')
- w_gate: bfloat16 [1, 1024, 4096], P(None, 'dp')
- w_up: bfloat16 [1, 1024, 4096], P(None, 'dp')
- w_down: bfloat16 [1, 4096, 1024], P(None, 'dp')
Outputs:
- output 1: bfloat16 [256, 2048, 1024], P(('rep', 'dp')), parts along dimension 0
- output 2: bfloat16 [2, 1024, 1024], P('rep', 'dp'), parts along dimension 0
- output 3: bfloat16 [2, 1024, 1024], P('rep', 'dp'), parts along dimension 0
- output 4: bfloat16 [2, 1024, 1024], P('rep', 'dp'), parts along dimension 0
- output 5: bfloat16 [2, 1024, 1024], P('rep', 'dp'), parts along dimension 0
- output 6: bfloat16 [2, 1024, 4096], P('rep', 'dp'), parts along dimension 0
- output 7: bfloat16 [2, 1024, 4096], P('rep', 'dp'), parts along dimension 0
- output 8: bfloat16 [2, 4096, 1024], P('rep', 'dp'), parts along dimension 0
There are 2 independent parts. The reference program is written for one: setup_inputs(seed, part) draws one part's arguments, and reference() takes and returns one part's arrays. A program takes and returns all parts, laid end to end along the dimension named above; an argument that names none is the same for every part.
All inputs are finite; a program needn't handle non-finite values.
Results may differ from the reference program's by a relative error of at most 0.0293.
Values are sent between devices in bfloat16 or wider.
A program may use at most 768 MiB of HBM per device.

```python
import jax
import jax.numpy as jnp
from jax import lax

SEQUENCES = 128
TOKENS = 2048
D = 1024
HEADS = 4
KV_HEADS = 4
HEAD = 256
FF = 4096
LAYERS = 1
THETA = 10000
NAMES = ("wq", "wk", "wv", "wo", "w_gate", "w_up", "w_down")
SHAPES = {
    "wq": (LAYERS, D, HEADS * HEAD),
    "wk": (LAYERS, D, KV_HEADS * HEAD),
    "wv": (LAYERS, D, KV_HEADS * HEAD),
    "wo": (LAYERS, HEADS * HEAD, D),
    "w_gate": (LAYERS, D, FF),
    "w_up": (LAYERS, D, FF),
    "w_down": (LAYERS, FF, D),
}


def bump(key, n, height):
    away = (jnp.arange(n, dtype=jnp.int32) - jax.random.randint(key, (), 0, n, jnp.int32)) % n
    return jnp.where(away < n // 8, height, 1.0)


def together(key, own, strength):
    shared = jax.random.normal(key, own.shape[1:], jnp.float32)
    return (own + strength * shared) * lax.rsqrt(1 + strength * strength)


def setup_inputs(seed: int = 0, part: int = 0) -> dict:
    kx, kdy, ka, kb, kz, kf, kh, kl, *keys = jax.random.split(jax.random.key(seed), 8 + 3 * len(NAMES))
    kx, kdy, ka, kb = (jax.random.fold_in(k, part) for k in (kx, kdy, ka, kb))
    kw, km, kv = (keys[i::3] for i in range(3))
    shape = (SEQUENCES, TOKENS, D)
    much_x, much_dy = jax.random.uniform(kz, (2,), jnp.float32, 0.0, 1.0)
    loud = 2.0 ** jax.random.uniform(jax.random.fold_in(kz, 1), (), jnp.float32, -1.0, 2.0)
    layers = 2.0 ** jax.random.uniform(kl, (LAYERS, 1, 1), jnp.float32, -1.0, 1.0)
    times = {"wq": 1.0, "wk": 1.0, "wv": 2.0, "wo": layers, "w_gate": 1.0, "w_up": bump(kh, FF, 4.0), "w_down": layers}
    x = together(ka, jax.random.normal(kx, shape, jnp.float32), much_x) * bump(kf, D, 4.0)
    dy = together(kb, jax.random.normal(kdy, shape, jnp.float32), much_dy)
    drawn = {"x": x.astype(jnp.bfloat16), "dy": (loud * dy * (SEQUENCES * TOKENS) ** -0.5).astype(jnp.bfloat16)}
    for key, name in zip(kw, NAMES, strict=True):
        drawn[name] = (jax.random.normal(key, SHAPES[name], jnp.float32) * SHAPES[name][1] ** -0.5 * times[name]).astype(jnp.bfloat16)
    return drawn


def matmul(a, w):
    return jnp.dot(a, w, preferred_element_type=jnp.float32).astype(jnp.bfloat16)


def normed(h):
    wide = h.astype(jnp.float32)
    scale = lax.rsqrt(jnp.mean(wide**2, -1, keepdims=True) + 1e-6)
    return (wide * scale).astype(jnp.bfloat16)


def turned(t, theta):
    half = t.shape[-1] // 2
    angle = jnp.arange(t.shape[0], dtype=jnp.float32)[:, None] * theta ** (-jnp.arange(half, dtype=jnp.float32) / half)
    cos, sin = jnp.cos(angle)[:, None], jnp.sin(angle)[:, None]
    a, b = t[..., :half].astype(jnp.float32), t[..., half:].astype(jnp.float32)
    return jnp.concatenate([a * cos - b * sin, b * cos + a * sin], -1).astype(jnp.bfloat16)


def seen_by(q, k, v):
    tokens, kv = q.shape[0], k.shape[1]
    q = q.reshape(tokens, kv, -1, q.shape[-1])
    scores = jnp.einsum("tgsd,ugd->gstu", q.astype(jnp.float32), k.astype(jnp.float32)) * q.shape[-1] ** -0.5
    place = jnp.arange(tokens)
    weights = jax.nn.softmax(jnp.where(place[:, None] >= place, scores, -jnp.inf), -1).astype(jnp.bfloat16)
    return jnp.einsum("gstu,ugd->tgsd", weights.astype(jnp.float32), v.astype(jnp.float32)).astype(jnp.bfloat16).reshape(tokens, -1)


def layer(h, w):
    a = normed(h)
    q, k = (turned(matmul(a, w[name]).reshape(h.shape[0], -1, HEAD), THETA) for name in ("wq", "wk"))
    h = h + matmul(seen_by(q, k, matmul(a, w["wv"]).reshape(h.shape[0], -1, HEAD)), w["wo"])
    b = normed(h)
    gate = jnp.dot(b, w["w_gate"], preferred_element_type=jnp.float32)
    up = jnp.dot(b, w["w_up"], preferred_element_type=jnp.float32)
    return h + matmul((jax.nn.silu(gate) * up).astype(jnp.bfloat16), w["w_down"])


def stack(weights, h):
    return lax.scan(lambda h, w: (layer(h, w), None), h, weights)[0]


def reference(x, dy, wq, wk, wv, wo, w_gate, w_up, w_down):
    weights = dict(zip(NAMES, (wq, wk, wv, wo, w_gate, w_up, w_down), strict=True))

    def take(so_far, sequence):
        h, by_y = sequence
        _, back = jax.vjp(stack, weights, h)
        by_weights, by_h = back(by_y)
        return jax.tree.map(lambda total, term: total + term.astype(jnp.float32), so_far, by_weights), by_h

    none_yet = {name: jnp.zeros(w.shape, jnp.float32) for name, w in weights.items()}
    by_weights, by_x = lax.scan(take, none_yet, (x, dy))
    return (by_x, *(by_weights[name].astype(jnp.bfloat16) for name in NAMES))
```

```python
import functools

import jax
import jax.numpy as jnp
from jax import lax
from jax.experimental import pallas as pl
from jax.experimental.pallas import tpu as pltpu
from jax.sharding import Mesh
from jax.sharding import PartitionSpec as P

HEAD = 256
HALF = HEAD // 2
THETA = 10000
NEG = -1e30
HIDDEN = 2 * NEG
LOG2E = 1.4426950408889634
VMEM = 62 * 2**20
BLOCK = 512
PAIR = 2 * HEAD
SCALE = HEAD**-0.5
BF = jnp.bfloat16
F32 = jnp.float32


def _dot(a, b, turned=False):
    return lax.dot_general(a, b, (((1,), (int(turned),)), ((), ())), preferred_element_type=F32)


def _dot_t(a, b):
    return _dot(a, b, True)


def _loop(n, body):
    lax.fori_loop(0, n, body, None)


def _params(semantics):
    return pltpu.CompilerParams(dimension_semantics=semantics, vmem_limit_bytes=VMEM)


def _once(shape, index):
    return pl.BlockSpec(shape, index, pipeline_mode=pl.Buffered(1))


def _turn(t, cos, sin):
    a, b = t[:, :HALF], t[:, HALF:]
    return jnp.concatenate([a * cos - b * sin, b * cos + a * sin], 1).astype(BF)


def _turn_back(t, cos, sin):
    a, b = t[:, :HALF], t[:, HALF:]
    return jnp.concatenate([a * cos + b * sin, b * cos - a * sin], 1).astype(BF)


def _project(a_ref, w_ref, cos_ref, sin_ref, out_ref):
    cos, sin = cos_ref[:], sin_ref[:]
    for p in range(2):
        for part in range(3):
            at = part * PAIR
            t = _dot(a_ref[:], w_ref[p, :, at : at + PAIR]).astype(BF)
            if part < 2:
                for h in range(2):
                    one = t[:, h * HEAD : (h + 1) * HEAD].astype(F32)
                    out_ref[p, :, at + h * HEAD : at + (h + 1) * HEAD] = _turn(one, cos, sin)
            else:
                out_ref[p, :, at : at + PAIR] = t


def project(a, w, cos, sin, block=BLOCK):
    tokens, d = a.shape
    block = min(block, tokens)
    wide = 3 * PAIR
    rows = lambda i: (i, 0)
    return pl.pallas_call(
        _project,
        grid=(tokens // block,),
        in_specs=[pl.BlockSpec((block, d), rows), _once((2, d, wide), lambda i: (0, 0, 0)), pl.BlockSpec((block, HALF), rows), pl.BlockSpec((block, HALF), rows)],
        out_specs=pl.BlockSpec((2, block, wide), lambda i: (0, i, 0)),
        out_shape=jax.ShapeDtypeStruct((2, tokens, wide), BF),
        compiler_params=_params(("arbitrary",)),
        name="project",
    )(a, w, cos, sin)


def _gap(bk, bq):
    return lax.broadcasted_iota(jnp.int32, (bk, bq), 1) - lax.broadcasted_iota(jnp.int32, (bk, bq), 0)


def _forward(q_ref, k_ref, v_ref, o_ref, ot_ref, lse_ref, top_s, mix_s):
    bq = q_ref.shape[1]
    iq = pl.program_id(0)
    e = SCALE * LOG2E
    heads = [(h // 2, slice((h % 2) * HEAD, (h % 2 + 1) * HEAD)) for h in range(4)]
    top_s[:] = jnp.full(top_s.shape, NEG, F32)
    mix_s[:] = jnp.zeros(mix_s.shape, F32)
    ones = jnp.ones((8, bq), BF)

    def block(j, masked):
        here = pl.ds(pl.multiple_of(j * bq, bq), bq)
        scores = [_dot_t(k_ref[p, here, at], q_ref[p, :, at]) for p, at in heads]
        weights, keeps = [], []
        for h, s in enumerate(scores):
            if masked:
                s = jnp.where(_gap(bq, bq) >= 0, s, HIDDEN)
            old = top_s[h : h + 1, :]
            top = jnp.maximum(old, s.max(axis=0, keepdims=True))
            top_s[h : h + 1, :] = top
            weights.append(jnp.exp2((s - top) * e).astype(BF))
            keeps.append(jnp.exp2((old - top) * e))
        for h, (p, at) in enumerate(heads):
            values = jnp.concatenate([v_ref[p, here, at].T, ones], axis=0)
            mix_s[h] = mix_s[h] * keeps[h] + _dot(values, weights[h])

    _loop(iq, lambda j, _: block(j, False))
    block(iq, True)
    for h in range(4):
        total = mix_s[h, HEAD : HEAD + 1, :]
        out = (mix_s[h, :HEAD, :] * (1 / total)).astype(BF)
        ot_ref[h * HEAD : (h + 1) * HEAD, :] = out
        o_ref[:, h * HEAD : (h + 1) * HEAD] = out.T
        lse_ref[h : h + 1, :] = top_s[h : h + 1, :] * SCALE + jnp.log(total)


def attend(qkv, block=BLOCK):
    tokens = qkv.shape[1]
    block = min(block, tokens)
    return pl.pallas_call(
        _forward,
        grid=(tokens // block,),
        in_specs=[pl.BlockSpec((2, block, PAIR), lambda i: (0, i, 0)), _once((2, tokens, PAIR), lambda i: (0, 0, 1)), _once((2, tokens, PAIR), lambda i: (0, 0, 2))],
        out_specs=[pl.BlockSpec((block, 2 * PAIR), lambda i: (i, 0)), pl.BlockSpec((2 * PAIR, block), lambda i: (0, i)), pl.BlockSpec((4, block), lambda i: (0, i))],
        out_shape=[jax.ShapeDtypeStruct((tokens, 2 * PAIR), BF), jax.ShapeDtypeStruct((2 * PAIR, tokens), BF), jax.ShapeDtypeStruct((4, tokens), F32)],
        scratch_shapes=[pltpu.VMEM((4, block), F32), pltpu.VMEM((4, HEAD + 8, block), F32)],
        compiler_params=_params(("arbitrary",)),
        name="attend",
    )(qkv, qkv, qkv)


def _backward(q_ref, k_ref, v_ref, do_ref, lse_ref, delta_ref, cos_ref, sin_ref, out_ref, dq_s, dk_s, dv_s, *, wide):
    bq = q_ref.shape[1]
    iq = pl.program_id(1)
    e = SCALE * LOG2E
    pieces = [(h, at) for at in range(0, bq, wide) for h in range(2)]
    mine = [slice(h * HEAD, (h + 1) * HEAD) for h in range(2)]

    @pl.when(iq == 0)
    def _():
        dk_s[:] = jnp.zeros_like(dk_s)
        dv_s[:] = jnp.zeros_like(dv_s)

    dq_s[:] = jnp.zeros_like(dq_s)

    def block(j, masked):
        here = pl.ds(pl.multiple_of(j * bq, bq), bq)
        qs = [q_ref[0, at : at + wide, mine[h]] for h, at in pieces]
        dos = [do_ref[at : at + wide, mine[h]] for h, at in pieces]
        scores = [_dot_t(k_ref[0, here, mine[h]], x) for (h, _), x in zip(pieces, qs)]
        dps = [_dot_t(v_ref[0, here, mine[h]], x) for (h, _), x in zip(pieces, dos)]
        for n, (h, at) in enumerate(pieces):
            p = jnp.exp2(scores[n] * e - lse_ref[0, h : h + 1, at : at + wide] * LOG2E)
            if masked:
                p = jnp.where(_gap(bq, wide) >= -at, p, 0.0)
            ds = (p * (dps[n] - delta_ref[0, h : h + 1, at : at + wide])).astype(BF)
            dv_s[here, mine[h]] += _dot(p.astype(BF), dos[n])
            dk_s[here, mine[h]] += _dot(ds, qs[n])
            dq_s[h, :, at : at + wide] += _dot(k_ref[0, here, mine[h]].T, ds)

    _loop(iq, lambda j, _: block(j, False))
    block(iq, True)
    rows = pl.ds(pl.multiple_of(iq * bq, bq), bq)
    cos, sin = cos_ref[rows, :], sin_ref[rows, :]
    for h in range(2):
        out_ref[0, rows, mine[h]] = _turn_back((dq_s[h] * SCALE).astype(BF).T.astype(F32), cos, sin)

    @pl.when(iq == pl.num_programs(1) - 1)
    def _():
        def finish(j, _):
            here = pl.ds(pl.multiple_of(j * bq, bq), bq)
            for h in range(2):
                dk = (dk_s[here, mine[h]] * SCALE).astype(BF).astype(F32)
                out_ref[0, here, (2 + h) * HEAD : (3 + h) * HEAD] = _turn_back(dk, cos_ref[here, :], sin_ref[here, :])
                out_ref[0, here, (4 + h) * HEAD : (5 + h) * HEAD] = dv_s[here, mine[h]].astype(BF)

        _loop(pl.num_programs(1), finish)


def attend_bwd(qkv, d_out, lse, delta, cos, sin, block=BLOCK, wide=256):
    tokens = qkv.shape[1]
    block = min(block, tokens)
    wide = min(wide, block)
    whole = lambda p, i: (0, 0)
    stats = pl.BlockSpec((1, 2, block), lambda p, i: (p, 0, i))
    return pl.pallas_call(
        functools.partial(_backward, wide=wide),
        grid=(2, tokens // block),
        in_specs=[pl.BlockSpec((1, block, PAIR), lambda p, i: (p, i, 0)), _once((1, tokens, PAIR), lambda p, i: (p, 0, 1)), _once((1, tokens, PAIR), lambda p, i: (p, 0, 2)),
                  pl.BlockSpec((block, PAIR), lambda p, i: (i, p)), stats, stats, _once((tokens, HALF), whole), _once((tokens, HALF), whole)],
        out_specs=pl.BlockSpec((1, tokens, 3 * PAIR), lambda p, i: (p, 0, 0)),
        out_shape=jax.ShapeDtypeStruct((2, tokens, 3 * PAIR), BF),
        scratch_shapes=[pltpu.VMEM((2, HEAD, block), F32), pltpu.VMEM((tokens, PAIR), F32), pltpu.VMEM((tokens, PAIR), F32)],
        compiler_params=_params(("arbitrary", "arbitrary")),
        name="attend_bwd",
    )(qkv, qkv, qkv, d_out, lse, delta, cos, sin)


def _feed(*refs, first, block):
    b_ref, bt_ref, dy_ref, dyt_ref, gu_ref, wd_ref, *rest = refs
    if not first:
        before_ref, _, *rest = rest
    dgu_ref, dwd_ref, db_ref, db_s, g_s, u_s, d_s, sem = rest
    j = pl.program_id(0)
    tokens = b_ref.shape[0]
    hidden = wd_ref.shape[1]
    half = wd_ref.shape[2]

    @pl.when(j == 0)
    def _():
        if first:
            db_s[:] = jnp.zeros_like(db_s)
        else:
            copy = pltpu.make_async_copy(before_ref, db_s, sem)
            copy.start()
            copy.wait()

    g_s[:] = jnp.zeros_like(g_s)
    u_s[:] = jnp.zeros_like(u_s)
    d_s[:] = jnp.zeros_like(d_s)

    def step(i, _):
        rows = pl.ds(pl.multiple_of(i * block, block), block)
        b, dy = b_ref[rows, :], dy_ref[rows, :]
        gate = _dot(b, gu_ref[0])
        up = _dot(b, gu_ref[1])
        by_act = (_dot_t(dy[:, :half], wd_ref[0]) + _dot_t(dy[:, half:], wd_ref[1])).astype(BF).astype(F32)
        sig = 1 / (1 + jnp.exp(-gate))
        silu = gate * sig
        act = (silu * up).astype(BF)
        by_up = (by_act * silu).astype(BF)
        by_gate = (by_act * up * (sig + silu * (1 - sig))).astype(BF)
        db_s[rows, :] += _dot_t(by_gate, gu_ref[0]) + _dot_t(by_up, gu_ref[1])
        g_s[:] += _dot(bt_ref[:, rows], by_gate)
        u_s[:] += _dot(bt_ref[:, rows], by_up)
        d_s[:] += _dot(dyt_ref[:, rows], act)
        return None

    _loop(tokens // block, step)
    dgu_ref[:, :hidden] = g_s[:].astype(BF)
    dgu_ref[:, hidden:] = u_s[:].astype(BF)
    dwd_ref[:] = d_s[:].T.astype(BF)

    @pl.when(j == pl.num_programs(0) - 1)
    def _():
        copy = pltpu.make_async_copy(db_s, db_ref, sem)
        copy.start()
        copy.wait()


def feed(b, bt, dy, dyt, gu, wd, at, before=None, hidden=BLOCK, block=BLOCK):
    tokens, d = b.shape
    units = gu.shape[2]
    hidden, block = min(hidden, units), min(block, tokens)
    whole = lambda j: (0, 0)
    any_ = pl.BlockSpec(memory_space=pl.ANY)
    specs = [_once((tokens, d), whole), _once((d, tokens), whole), _once((tokens, d), whole), _once((d, tokens), whole),
             pl.BlockSpec((2, d, hidden), lambda j: (0, 0, j)), pl.BlockSpec((2, hidden, d // 2), lambda j: (0, at // hidden + j, 0))]
    args = [b, bt, dy, dyt, gu, wd]
    if before is not None:
        specs += [any_, any_]
        args += [before[1], before[0]]
    return pl.pallas_call(
        functools.partial(_feed, first=before is None, block=block),
        grid=(units // hidden,),
        in_specs=specs,
        out_specs=[pl.BlockSpec((d, 2 * hidden), lambda j: (0, j)), pl.BlockSpec((hidden, d), lambda j: (at // hidden + j, 0)), any_],
        out_shape=[jax.ShapeDtypeStruct((d, 2 * units), BF), jax.ShapeDtypeStruct((wd.shape[1], d), BF), jax.ShapeDtypeStruct((tokens, d), F32)],
        scratch_shapes=[pltpu.VMEM((tokens, d), F32), pltpu.VMEM((d, hidden), F32), pltpu.VMEM((d, hidden), F32), pltpu.VMEM((d, hidden), F32),
                        pltpu.SemaphoreType.DMA],
        input_output_aliases={} if before is None else {7: 1},
        compiler_params=_params(("arbitrary",)),
        name="feed",
    )(*args)


ORDERS = (("x", "y", "z"), ("y", "z", "x"), ("z", "x", "y"))
LATENCY = 0.03
ROUTES = 2


def _timetable(sizes, growing=False):
    events = []
    for o, order in enumerate(ORDERS):
        counts = [sizes[axis] for axis in order]
        at, left, step = 0, 1, 0
        if growing:
            left /= counts[0] * counts[1] * counts[2]
        for n in counts:
            for _ in range(n - 1):
                events.append((at, step, o))
                at += LATENCY + (left if growing else left / n)
                step += 1
            left = left * n if growing else left / n
        events.append((at, step, o))
    return [(o, step) for _, step, o in sorted(events)]


def _reduce(*refs, sizes):
    g, out, own, got1, sum1, got2, sum2, got3, put2, put3, own_sem, send_sem, recv_sem = zip(*[iter(refs)] * 3)
    place = {axis: lax.axis_index(axis) for axis in sizes}

    barrier = pltpu.get_barrier_semaphore()
    for axis, n in sizes.items():
        for way in (1, n - 1):
            pl.semaphore_signal(barrier, 1, device_id={axis: lax.rem(place[axis] + way, n)}, device_id_type=pl.DeviceIdType.MESH)
    pl.semaphore_wait(barrier, 2 * len(sizes))

    def stage(o, step, way, m):
        order = ORDERS[o]
        n1, n2, n3 = (sizes[axis] for axis in order)
        wide = own[o].shape[-1]
        columns = pl.ds(pl.multiple_of(m * wide, wide), wide)
        rest = [axis for axis in ("x", "y", "z") if axis != order[0]]
        lead, turn = sizes[rest[0]], sizes[rest[1]]
        phase = 0 if step < n1 else 1 if step < n1 + n2 - 1 else 2
        before = (0, n1 - 1, n1 + n2 - 2, n1 + n2 + n3 - 3)

        def part(axis, t):
            n = sizes[axis]
            return lax.rem(place[axis] + jnp.where(way == 0, n - t - 1, t + 1), n)

        def source(c):
            index = [slice(None)] * 3
            index["xyz".index(order[0])] = c
            return g[o].at[(*index, slice(None), columns)]

        def load(t):
            return pltpu.make_async_copy(source(part(order[0], t)), own[o].at[m, t % 2], own_sem[o].at[m, t % 2])

        def send(from_ref, to_ref, axis, step):
            n = sizes[axis]
            after = lax.rem(place[axis] + jnp.where(way == 0, 1, n - 1), n)
            return pltpu.make_async_remote_copy(src_ref=from_ref, dst_ref=to_ref, send_sem=send_sem[o].at[m, step], recv_sem=recv_sem[o].at[m, step],
                                                device_id={axis: after}, device_id_type=pl.DeviceIdType.MESH)

        def buffer(step):
            if step < before[1]:
                return got1[o].at[m, step]
            if step < before[2]:
                return got2[o].at[m, step - before[1]]
            return got3[o].at[m, step - before[2]]

        def first(ref, c):
            return ref.at[m, c] if rest[0] == order[1] else ref.at[m, :, c]

        if step == 0:
            load(1).start()
            send(source(part(order[0], 0)), buffer(0), order[0], 0).start()
            return
        landed = buffer(step - 1)
        last_axis = order[0] if step - 1 < before[1] else order[1] if step - 1 < before[2] else order[2]
        send(landed, landed, last_axis, step - 1).wait_recv()

        if step <= before[1]:
            load(step).wait()
            if step < before[1]:
                load(step + 1).start()
            done = step == before[1]
            to = sum1[o].at[m] if done else landed

            def add(i, _):
                for v in range(turn):
                    total = landed[i, v].astype(F32) + own[o][m, step % 2, i, v].astype(F32)
                    to[i, v] = total if done else total.astype(BF)

            _loop(lead, add)
            if not done:
                send(landed, buffer(step), order[0], step).start()
                return
            c = part(order[1], 0)
            from_ref = first(sum1[o], c)
            for v in range(n3):
                put2[o][m, v] = from_ref[v].astype(BF)
            send(put2[o].at[m], buffer(step), order[1], step).start()
        elif step <= before[2]:
            t = step - before[1]
            done = step == before[2]
            from_ref = first(sum1[o], part(order[1], t))
            for v in range(n3):
                total = landed[v].astype(F32) + from_ref[v]
                if done:
                    sum2[o][m, v] = total
                else:
                    landed[v] = total.astype(BF)
            if not done:
                send(landed, buffer(step), order[1], step).start()
                return
            put3[o][m] = sum2[o][m, part(order[2], 0)].astype(BF)
            send(put3[o].at[m], buffer(step), order[2], step).start()
        else:
            t = step - before[2]
            total = (landed[:].astype(F32) + sum2[o][m, part(order[2], t)]).astype(BF)
            if step < before[3]:
                landed[:] = total
                send(landed, buffer(step), order[2], step).start()
            else:
                out[o][:, columns] = total

    def both(o, step, k):
        def one(way, _):
            stage(o, step, way, way * ROUTES + k)

        _loop(2, one)

    for o, step in _timetable(sizes):
        _loop(ROUTES, lambda k, _, o=o, step=step: both(o, step, k))

    for o, order in enumerate(ORDERS):
        def left(m, _, o=o, order=order):
            step = 0
            for axis, got in zip(order, (got1, got2, got3), strict=True):
                for t in range(sizes[axis] - 1):
                    ref = got[o].at[m, t]
                    pltpu.make_async_remote_copy(src_ref=ref, dst_ref=ref, send_sem=send_sem[o].at[m, step], recv_sem=recv_sem[o].at[m, step],
                                                 device_id={axis: place[axis]}, device_id_type=pl.DeviceIdType.MESH).wait_send()
                    step += 1

        _loop(2 * ROUTES, left)


def reduce(arrays, sizes):
    shape = tuple(sizes.values())
    rings = 2 * ROUTES
    parts = [(t.shape[3], t.shape[4] // rings) for t in arrays]
    steps = sum(shape) - 3

    def per_array(make):
        made = []
        for order, (rows, wide) in zip(ORDERS, parts, strict=True):
            rest = [n for axis, n in sizes.items() if axis != order[0]]
            made.append(make([sizes[axis] for axis in order], rest, rows, wide))
        return made

    scratch = [
        *per_array(lambda n, rest, rows, wide: pltpu.VMEM((rings, 2, *rest, rows, wide), BF)),
        *per_array(lambda n, rest, rows, wide: pltpu.VMEM((rings, n[0] - 1, *rest, rows, wide), BF)),
        *per_array(lambda n, rest, rows, wide: pltpu.VMEM((rings, *rest, rows, wide), F32)),
        *per_array(lambda n, rest, rows, wide: pltpu.VMEM((rings, n[1] - 1, n[2], rows, wide), BF)),
        *per_array(lambda n, rest, rows, wide: pltpu.VMEM((rings, n[2], rows, wide), F32)),
        *per_array(lambda n, rest, rows, wide: pltpu.VMEM((rings, n[2] - 1, rows, wide), BF)),
        *per_array(lambda n, rest, rows, wide: pltpu.VMEM((rings, n[2], rows, wide), BF)),
        *per_array(lambda n, rest, rows, wide: pltpu.VMEM((rings, rows, wide), BF)),
        *(pltpu.SemaphoreType.DMA((rings, 2)),) * 3,
        *(pltpu.SemaphoreType.DMA((rings, steps)),) * 6,
    ]
    size = sum(t.size for t in arrays) * 2
    return pl.pallas_call(
        functools.partial(_reduce, sizes=sizes),
        in_specs=[pl.BlockSpec(memory_space=pl.ANY)] * 3,
        out_specs=[pl.BlockSpec(memory_space=pltpu.VMEM)] * 3,
        out_shape=[jax.ShapeDtypeStruct(t.shape[3:], BF) for t in arrays],
        scratch_shapes=scratch,
        compiler_params=pltpu.CompilerParams(collective_id=0, has_side_effects=True, vmem_limit_bytes=VMEM),
        name="reduce",
    )(*arrays)


QUARTERS = (slice(1), slice(2, 4), slice(1, 2))


def _gather(*refs, sizes):
    given, out, held = refs[:4], refs[4:8], refs[8:12]
    load_sem, send_sem, recv_sem, out_sem, hand_sem, pair_sem = refs[12:]
    place = {axis: lax.axis_index(axis) for axis in sizes}
    me = lax.axis_index("rep")
    at = tuple(place.values())

    barrier = pltpu.get_barrier_semaphore()
    for axis, n in sizes.items():
        for way in (1, n - 1):
            pl.semaphore_signal(barrier, 1, device_id={axis: lax.rem(place[axis] + way, n)}, device_id_type=pl.DeviceIdType.MESH)
    pl.semaphore_signal(barrier, 1, device_id={"rep": 1 - me}, device_id_type=pl.DeviceIdType.MESH)
    loads = [pltpu.make_async_copy(ref, to.at[at], load_sem.at[i]) for i, (ref, to) in enumerate(zip(given, held))]
    for load in loads:
        load.start()
    for load in loads:
        load.wait()
    pl.semaphore_wait(barrier, 2 * len(sizes) + 1)

    def ring(o, step, way, route, finish=False):
        order = ORDERS[o]
        counts = [sizes[axis] for axis in order]
        before = [sum(counts[:i]) - i for i in range(4)]
        last = route is None
        m = 2 * ROUTES + way if last else way * ROUTES + route
        which = 3 if last else o
        wide = held[which].shape[-1] // (2 if last else 2 * ROUTES)
        columns = pl.ds(pl.multiple_of((way if last else m) * wide, wide), wide)
        tail = (QUARTERS[o], slice(None), columns) if last else (slice(None), columns)

        def chunk(phase, t):
            index = dict(place)
            for axis in order[:phase]:
                index[axis] = slice(None)
            n = counts[phase]
            index[order[phase]] = lax.rem(place[order[phase]] + jnp.where(way == 0, n - t, t), n)
            return (*index.values(), *tail)

        def copy(step):
            phase = 0 if step < before[1] else 1 if step < before[2] else 2
            axis = order[phase]
            n = counts[phase]
            after = lax.rem(place[axis] + jnp.where(way == 0, 1, n - 1), n)
            sent = held[which].at[chunk(phase, step - before[phase])]
            return pltpu.make_async_remote_copy(src_ref=sent, dst_ref=sent, send_sem=send_sem.at[o, m, step], recv_sem=recv_sem.at[o, m, step],
                                                device_id={axis: after}, device_id_type=pl.DeviceIdType.MESH)

        def arrived(step):
            phase = 0 if step < before[1] else 1 if step < before[2] else 2
            ref = held[which].at[chunk(phase, step - before[phase] + 1)]
            return pltpu.make_async_remote_copy(src_ref=ref, dst_ref=ref, send_sem=send_sem.at[o, m, step], recv_sem=recv_sem.at[o, m, step],
                                                device_id={"rep": me}, device_id_type=pl.DeviceIdType.MESH)

        def mine(t):
            index = chunk(2, t)
            return pltpu.make_async_copy(held[which].at[index], out[which].at[(me, *index)], out_sem.at[o, m, t])

        def hand(t):
            index = chunk(2, t)
            return pltpu.make_async_remote_copy(src_ref=held[which].at[index], dst_ref=out[which].at[(me, *index)], send_sem=hand_sem.at[o, m, t],
                                                recv_sem=pair_sem.at[o, m, t], device_id={"rep": 1 - me}, device_id_type=pl.DeviceIdType.MESH)

        def theirs(t):
            ref = out[which].at[(1 - me, *chunk(2, t))]
            return pltpu.make_async_remote_copy(src_ref=ref, dst_ref=ref, send_sem=hand_sem.at[o, m, t], recv_sem=pair_sem.at[o, m, t],
                                                device_id={"rep": 1 - me}, device_id_type=pl.DeviceIdType.MESH)

        if finish:
            for t in range(before[3]):
                copy(t).wait_send()
            for t in range(counts[2]):
                mine(t).wait()
                hand(t).wait_send()
                theirs(t).wait_recv()
            return
        if step > 0:
            arrived(step - 1).wait_recv()
        if step < before[3]:
            copy(step).start()
        if step >= before[2]:
            mine(step - before[2]).start()
            hand(step - before[2]).start()

    def every(o, step, **how):
        def one(way, _):
            _loop(ROUTES, lambda k, _: ring(o, step, way, k, **how))
            ring(o, step, way, None, **how)

        _loop(2, one)

    for o, step in _timetable(sizes, growing=True):
        every(o, step)
    for o in range(3):
        every(o, 0, finish=True)


def gather(blocks, sizes):
    shape = tuple(sizes.values())
    rings, steps = 2 * ROUTES + 2, sum(shape) - 3
    size = sum(t.size for t in blocks) * 2 * shape[0] * shape[1] * shape[2]
    sems = pltpu.SemaphoreType.DMA((3, rings, steps))
    ends = pltpu.SemaphoreType.DMA((3, rings, max(shape)))
    return pl.pallas_call(
        functools.partial(_gather, sizes=sizes),
        in_specs=[pl.BlockSpec(memory_space=pl.ANY)] * 4,
        out_specs=[pl.BlockSpec(memory_space=pl.ANY)] * 4,
        out_shape=[jax.ShapeDtypeStruct((2, *shape, *t.shape), BF) for t in blocks],
        scratch_shapes=[*(pltpu.VMEM((*shape, *t.shape), BF) for t in blocks), pltpu.SemaphoreType.DMA((4,)), sems, sems, ends, ends, ends],
        compiler_params=pltpu.CompilerParams(collective_id=1, has_side_effects=True, vmem_limit_bytes=VMEM),
        name="gather",
    )(*blocks)


def _statistic(wide):
    return lax.rsqrt(jnp.mean(wide * wide, -1, keepdims=True) + 1e-6)


def _normed_back(wide, by):
    scale = _statistic(wide)
    return by * scale - wide * (scale * scale * scale * jnp.mean(by * wide, -1, keepdims=True))


def _rows(kernel, args, specs, outs):
    tokens = args[0].shape[-2]
    block = min(BLOCK, tokens)

    def spec(kind, shape):
        if kind == "rows":
            return pl.BlockSpec((*shape[:-2], block, shape[-1]), lambda i: (*(0,) * (len(shape) - 2), i, 0))
        return pl.BlockSpec((*shape[:-1], block), lambda i: (*(0,) * (len(shape) - 1), i)) if kind == "columns" else kind

    shapes = [jax.ShapeDtypeStruct(shape, dtype) for _, shape, dtype in outs]
    return pl.pallas_call(
        kernel,
        grid=(tokens // block,),
        in_specs=[spec(kind, t.shape) for kind, t in zip(specs, args, strict=True)],
        out_specs=[spec(kind, shape) for kind, shape, _ in outs],
        out_shape=shapes,
        compiler_params=_params(("arbitrary",)),
    )(*args)


def _prepare(x_ref, dy_ref, a_ref, at_ref, dyt_ref):
    wide = x_ref[:].astype(F32)
    a = (wide * _statistic(wide)).astype(BF)
    a_ref[:] = a
    at_ref[:] = a.T
    dyt_ref[:] = dy_ref[:].T


def prepare(x, dy):
    tokens, d = x.shape
    flat, turned = ("rows", (tokens, d), BF), ("columns", (d, tokens), BF)
    return _rows(_prepare, (x, dy), ("rows", "rows"), (flat, turned, turned))


def _leave(x_ref, out_ref, wo_ref, h_ref, b_ref, bt_ref):
    half = wo_ref.shape[2]
    for p in range(2):
        at = slice(p * half, (p + 1) * half)
        h_ref[:, at] = (x_ref[:, at].astype(F32) + _dot(out_ref[:], wo_ref[p]).astype(BF).astype(F32)).astype(BF)
    wide = h_ref[:].astype(F32)
    b = (wide * _statistic(wide)).astype(BF)
    b_ref[:] = b
    bt_ref[:] = b.T


def _wo(w):
    d = w.shape[1]
    return _once((2, d, d // 2), lambda i: (0, 0, 3 * HEAD * 2 // (d // 2)))


def leave(x, out, w):
    tokens, d = x.shape
    flat, turned = ("rows", (tokens, d), BF), ("columns", (d, tokens), BF)
    return _rows(_leave, (x, out, w), ("rows", "rows", _wo(w)), (flat, flat, turned))


def _enter(db_ref, h_ref, dy_ref, out_ref, wo_ref, by_h_ref, by_out_ref, delta_ref):
    half = wo_ref.shape[2]
    by_h = (dy_ref[:].astype(F32) + _normed_back(h_ref[:].astype(F32), db_ref[:])).astype(BF)
    by_h_ref[:] = by_h
    by_out = (_dot_t(by_h[:, :half], wo_ref[0]) + _dot_t(by_h[:, half:], wo_ref[1])).astype(BF)
    by_out_ref[:] = by_out
    for h in range(4):
        at = slice(h * HEAD, (h + 1) * HEAD)
        t = by_out[:, at].astype(F32) * out_ref[:, at].astype(F32)
        delta_ref[h // 2, h % 2 : h % 2 + 1, :] = (t[:, :HALF] + t[:, HALF:]).T.sum(0, keepdims=True)


def enter(db, h, dy, out, w):
    tokens, d = h.shape
    flat = ("rows", (tokens, d), BF)
    return _rows(_enter, (db, h, dy, out, w), (*["rows"] * 4, _wo(w)), (flat, flat, ("columns", (2, 2, tokens), F32)))


def _inner(at_ref, ot_ref, by_qkv_ref, by_h_ref, out_ref, *, block):
    j = pl.program_id(0)

    def fill(left_ref, right):
        def some(i, _):
            rows = pl.ds(pl.multiple_of(i * block, block), block)
            out_ref[rows, :] = _dot(left_ref[rows, :], right()).astype(BF)

        _loop(out_ref.shape[0] // block, some)

    pl.when(j < 6)(lambda: fill(at_ref, lambda: by_qkv_ref[0]))
    pl.when(j >= 6)(lambda: fill(ot_ref, lambda: by_h_ref[:]))


def inner(at, ot, by_qkv, by_h):
    d, tokens = at.shape
    wide = PAIR
    whole = lambda j: (0, 0)
    return pl.pallas_call(
        functools.partial(_inner, block=BLOCK),
        grid=(8,),
        in_specs=[_once((d, tokens), whole), _once((d, tokens), whole), pl.BlockSpec((1, tokens, wide), lambda j: (jnp.minimum(j, 5) // 3, 0, jnp.minimum(j, 5) % 3)),
                  pl.BlockSpec((tokens, wide), lambda j: (0, jnp.maximum(j - 6, 0)))],
        out_specs=pl.BlockSpec((d, wide), lambda j: (0, j)),
        out_shape=jax.ShapeDtypeStruct((d, 8 * wide), BF),
        compiler_params=_params(("arbitrary",)),
        name="inner",
    )(at, ot, by_qkv, by_h)


def _finish(by_qkv_ref, w_ref, x_ref, by_h_ref, by_x_ref):
    by_a = _dot_t(by_qkv_ref[0], w_ref[0]) + _dot_t(by_qkv_ref[1], w_ref[1])
    by_x_ref[:] = (by_h_ref[:].astype(F32) + _normed_back(x_ref[:].astype(F32), by_a)).astype(BF)


def finish(by_qkv, w, x, by_h):
    tokens, d = x.shape
    columns = _once((2, d, 3 * PAIR), lambda i: (0, 0, 0))
    return _rows(_finish, (by_qkv, w, x, by_h), ("rows", columns, "rows", "rows"), (("rows", (tokens, d), BF),))[0]


def tables(tokens):
    angle = jnp.arange(tokens, dtype=F32)[:, None] * THETA ** (-jnp.arange(HALF, dtype=F32) / HALF)
    return jnp.cos(angle), jnp.sin(angle)


def solution(mesh):
    reps, group = mesh.devices.shape
    torus = {128: (4, 4, 8), 8: (2, 2, 2)}[group]
    grid = Mesh(mesh.devices.reshape(reps, *torus), ("rep", "x", "y", "z"))

    def step(x, dy, wq, wk, wv, wo, w_gate, w_up, w_down):
        x, dy = x[0], dy[0]
        tokens, d = x.shape
        units = w_gate.shape[2]
        part = units // 2
        second = lax.axis_index("rep") == 1

        def own(t):
            n = t.shape[1] // 2
            return jnp.where(second, t[:, n:], t[:, :n])

        sizes = dict(zip("xyz", torus, strict=True))
        blocks = [jnp.concatenate([own(t[0]) for t in (wq, wk, wv, wo)], 1)]
        blocks += [jnp.where(second, w_up[0, :, cut], w_gate[0, :, cut]) for cut in (slice(part), slice(part, units))]
        rows = w_down.shape[1]
        blocks += [own(w_down[0]).reshape(4, rows // 4, d // 2)]
        w_in, gu0, gu1, wd = (t.reshape(2, -1, t.shape[-1]) for t in gather(blocks, sizes))
        cos, sin = tables(tokens)

        a, at, dyt = prepare(x, dy)
        qkv = project(a, w_in, cos, sin)
        out, ot, lse = attend(qkv)
        h, b, bt = leave(x, out, w_in)

        dgu0, dwd, db = feed(b, bt, dy, dyt, gu0, wd, 0)
        dgu0 = lax.psum_scatter(dgu0, ("x", "y"), scatter_dimension=0, tiled=True)
        dgu1, dwd, db = feed(b, bt, dy, dyt, gu1, wd, part, (dwd, db))
        by_h, by_out, delta = enter(db, h, dy, out, w_in)
        by_qkv = attend_bwd(qkv, by_out, lse.reshape(2, 2, tokens), delta, cos, sin)
        d_in = inner(at, ot, by_qkv, by_h)
        by_x = finish(by_qkv, w_in, x, by_h)
        dgu0 = lax.psum_scatter(dgu0, "z", scatter_dimension=0, tiled=True)
        dgu1, by_down, ins = reduce([t.reshape(*torus, -1, t.shape[1]) for t in (dgu1, dwd, d_in)], sizes)

        rows = dgu0.shape[0]
        turns = jnp.stack([dgu0.reshape(rows, -1, 2, min(BLOCK, part)), dgu1.reshape(rows, -1, 2, min(BLOCK, part))], 1)
        by_gate, by_up = (turns[:, :, :, i].reshape(rows, units) for i in range(2))
        by_q, by_k, by_v = (jnp.concatenate([ins[:, i * PAIR : (i + 1) * PAIR], ins[:, (3 + i) * PAIR : (4 + i) * PAIR]], 1) for i in range(3))
        by_o = ins[:, 6 * PAIR :]
        return (by_x[None], *(t[None] for t in (by_q, by_k, by_v, by_o, by_gate, by_up, by_down)))

    states, cut = P(("rep", "x", "y", "z")), P(None, ("x", "y", "z"))
    return jax.shard_map(
        step,
        mesh=grid,
        in_specs=(states, states) + (cut,) * 7,
        out_specs=(states,) + (P("rep", ("x", "y", "z")),) * 7,
        check_vma=False,
    )
```
